128 devices in a mesh: dp: 64 (over y, z, x_lo, core), tensor: 2 (over x_hi).
Axes of the slice: x: 4 (x_hi: 2, x_lo: 2; x = x_hi * 2 + x_lo), y: 4, z: 4, core: 2. Of those that a mesh axis runs over, the one named last changes fastest.
Arguments:
- expert_act: bfloat16 [65536, 2880], P(('dp', 'tensor')), may hold values from -6 to 6
- grad_out: bfloat16 [131072, 1440], P(('dp', 'tensor')), may hold values from -6 to 6
- slot_token: int32 [65536], P(('dp', 'tensor')), may hold values from 0 to 1023, as said below
- slot_prob: float32 [65536], P(('dp', 'tensor')), may hold values from 0.2 to 1
- live_count: int32 [128], P(('dp', 'tensor')), may hold values from 128 to 512, as said below
Outputs:
- weight_grad: float32 [2880, 1440], P('dp', 'tensor')
The draws below stay inside these ranges and needn't reach their ends.
Inputs may be any that keep to these rules, and one draw needn't show every extreme that they name: `slot_token`: each device's 512 entries are distinct token indices of that device. `live_count`: each entry is 512 // j for some j of 1 to 4.
All inputs are finite; a program needn't handle non-finite values.
Results may differ from the reference program's by a relative error of at most 0.0029.
Values may be sent and summed in bfloat16 or wider, within the bound.
A program may use at most 128 MiB of HBM per device.

```python
import math
import jax
import jax.numpy as jnp
from jax import lax

D = 1440
FF = 2880
CAP = 512
TOK_DEV = 1024
SLOTS = 65536
TOKENS = 131072


def draw_slot_token(key, part):
    device_total = SLOTS // CAP
    device_keys = jax.random.split(jax.random.fold_in(key, 11), device_total)

    def shuffled(seed_key):
        return jax.random.permutation(seed_key, TOK_DEV)[:CAP].astype(jnp.int32)
    return jax.vmap(shuffled)(device_keys).reshape(-1).astype(jnp.int32)


def draw_live_count(key, part):
    device_total = SLOTS // CAP
    first_key = jax.random.fold_in(key, 21)
    second_key = jax.random.fold_in(key, 22)
    divisor = jax.random.randint(first_key, (device_total,), 1, 5)
    counted = (CAP // divisor).astype(jnp.int32)
    fullest = jax.random.randint(second_key, (), 0, device_total)
    return counted.at[fullest].set(CAP).astype(jnp.int32)


def block_levels(key, shape, shards, low, high):
    factor_of = 1.0
    for dim, blocks in shards:
        steps = jax.random.uniform(jax.random.fold_in(jax.random.fold_in(key, 6), dim), (blocks,), jnp.float32, low / len(shards), high / len(shards))
        factor_of = factor_of * jnp.repeat(jnp.exp(steps), shape[dim] // blocks).reshape((-1,) + (1,) * (len(shape) - 1 - dim))
    return factor_of


def normal_values(stream_key, dims, width, reach, pieces=(), kind=jnp.bfloat16):
    entries = jax.random.normal(stream_key, dims, jnp.float32) * width
    if len(pieces) > 0:
        entries = block_levels(stream_key, dims, pieces, -0.22, 0.18) * entries
    return jnp.clip(entries, min=-reach, max=reach).astype(kind)


def setup_inputs(seed: int = 0) -> dict:
    splits = jax.random.split(jax.random.key(seed), 6)
    expert_act = normal_values(splits[0], (SLOTS, FF), 1.0, 6.0, ((0, 128),))
    grad_out = normal_values(splits[1], (TOKENS, D), 1.0, 6.0, ((0, 128),))
    slot_token = draw_slot_token(jax.random.fold_in(splits[5], 71), 0)
    slot_prob = jnp.clip(jnp.exp(math.log(1.0) - 1.609438 * jax.random.uniform(splits[3], (SLOTS,), jnp.float32) ** block_levels(splits[3], (SLOTS,), ((0, 128),), -0.2, 0.2)), 0.2, 1.0)
    live_count = draw_live_count(jax.random.fold_in(splits[5], 71), 0)
    return dict(expert_act=expert_act, grad_out=grad_out, slot_token=slot_token, slot_prob=slot_prob, live_count=live_count)


def reference(expert_act, grad_out, slot_token, slot_prob, live_count):
    slot_total = expert_act.shape[0]
    position = jnp.arange(slot_total, dtype=jnp.int32)
    owner_dev = (position // CAP).astype(jnp.int32)
    token_rows = (slot_token + owner_dev * TOK_DEV).astype(jnp.int32)
    live_mask = position % CAP < live_count[owner_dev]
    weighting = jnp.where(live_mask, slot_prob, jnp.zeros_like(slot_prob))
    picked = grad_out[token_rows].astype(jnp.float32)
    weighted = (picked * weighting[:, None]).astype(jnp.bfloat16)
    gradient = lax.dot_general(expert_act, weighted, (((0,), (0,)), ((), ())), preferred_element_type=jnp.float32)
    return gradient * (1.0 / math.sqrt(slot_total))
```

```python
import functools
import math

import jax
import jax.numpy as jnp
from jax import lax
from jax.experimental import pallas as pl
from jax.experimental.pallas import tpu as pltpu
from jax.sharding import PartitionSpec as P

MESH = pl.DeviceIdType.MESH
F32, BF16 = jnp.float32, jnp.bfloat16
ROWS, PAD = 45, 48
WIDTHS = (256, 256, 208)
STARTS = (0, 256, 512)
HALF = 720
A_MSG, W_MSG, S1, S2, S3, N_MSG = 0, 1, 4, 22, 31, 40


def nt(left, right):
    return lax.dot_general(left, right, (((1,), (1,)), ((), ())), preferred_element_type=F32)


def kernel(
    scaling, tok_ref, prob_ref, live_ref, a_hbm, g_hbm, out_ref,
    a_v, g_v, hot, ap, ao, wp, wo, s1, r1, keep, acc, s2, r2, s3, r3,
    load_sem, send_sem, recv_sem,
):
    dp, x_hi = lax.axis_index("dp"), lax.axis_index("tensor")
    core = lax.rem(dp, 2)
    x_lo = lax.rem(lax.div(dp, 2), 2)
    z = lax.rem(lax.div(dp, 4), 4)
    y = lax.div(dp, 16)
    x = x_hi * 2 + x_lo

    def at(cx, cy, cz, cc):
        return (((cy * 4 + cz) * 2 + lax.rem(cx, 2)) * 2 + cc, lax.div(cx, 2))

    def moved(dim, by):
        place = {"x": x, "y": y, "z": z}
        place[dim] = lax.rem(place[dim] + by, 4)
        return at(place["x"], place["y"], place["z"], core)

    partner = at(x, y, z, 1 - core)
    here = {"x": x, "y": y, "z": z}
    orders = ("yzx", "zxy", "xyz")

    load_g = pltpu.make_async_copy(g_hbm, g_v, load_sem.at[0])
    load_a = pltpu.make_async_copy(a_hbm, a_v, load_sem.at[1])
    load_a.start()
    load_g.start()

    barrier = pltpu.get_barrier_semaphore()
    peers = [partner] + [moved(d, by) for d in "xyz" for by in (1, 2, 3)]
    for peer in peers:
        pl.semaphore_signal(barrier, inc=1, device_id=peer, device_id_type=MESH)

    sent = []

    def send(src, dst, index, device):
        copy = pltpu.make_async_remote_copy(
            src_ref=src, dst_ref=dst, send_sem=send_sem.at[index], recv_sem=recv_sem.at[index],
            device_id=device, device_id_type=MESH,
        )
        copy.start()
        sent.append(copy)
        return copy

    tokens, slots = hot.shape
    for start in range(0, tokens, 256):
        rows = lax.broadcasted_iota(jnp.int32, (256, slots), 0) + start
        hot[start : start + 256, :] = (rows == tok_ref[...]).astype(F32).astype(BF16)
    position = lax.broadcasted_iota(jnp.int32, (1, slots), 1)
    weighting = jnp.where(position < live_ref[0], prob_ref[...], jnp.zeros((1, slots), F32))

    load_a.wait()
    for parity in range(2):
        for q in range(32):
            first = ROWS * (2 * q + parity)
            base = first // 16 * 16
            stop = min(base + 64, a_v.shape[0])
            block = a_v[base:stop, :].astype(F32)[first - base : first - base + ROWS]
            block = jnp.concatenate([block, jnp.zeros((PAD - ROWS, slots), F32)], axis=0)
            ap[parity, q // 8, q // 2 % 4, q % 2] = block.astype(BF16)

    pl.semaphore_wait(barrier, len(peers))
    a_copy = send(ap.at[1 - core], ao, A_MSG, partner)

    load_g.wait()
    w_copies = []
    for k in range(3):
        width = WIDTHS[k]
        for half in range(2):
            first = half * HALF + STARTS[k]
            picked = jnp.dot(g_v[first : first + width, :], hot[...], preferred_element_type=F32)
            wp[k, half, :width, :] = (picked * weighting).astype(BF16)
            if width < 256:
                wp[k, half, width:, :] = jnp.zeros((256 - width, slots), BF16)
        w_copies.append(send(wp.at[k], wo.at[k], W_MSG + k, partner))

    a_copy.wait_recv()
    for copy in w_copies:
        copy.wait_recv()

    def unit(k, place, half):
        if k == 0:
            own, other, right = ap[core, place], ao[place], (k, half)
        elif k == 1:
            own, other, right = ap[core, :, place], ao[:, place], (k, half)
        else:
            low = lax.rem(place, 2)
            own = ap[core, 2 * half : 2 * half + 2, :, low]
            other = ao[2 * half : 2 * half + 2, :, low]
            right = (k, lax.div(place, 2))
        own, other = own.reshape(8 * PAD, slots), other.reshape(8 * PAD, slots)
        return (nt(own, wp[right]) + nt(other, wo[right])).reshape(8, PAD, 256)

    def first_stage(k, message, device):
        index = k * 6 + message
        return send(s1.at[k, message], r1.at[k, message], S1 + index, device)

    firsts = [[None] * 6 for _ in range(3)]
    for k in range(3):
        dim = orders[k][0]
        far = lax.rem(here[dim] + 2, 4)
        for half in range(2):
            s1[k, half] = unit(k, far, half).astype(BF16)
            firsts[k][half] = first_stage(k, half, moved(dim, 1 if half == 0 else 3))
    for k in range(3):
        dim = orders[k][0]
        up, down = lax.rem(here[dim] + 1, 4), lax.rem(here[dim] + 3, 4)
        s1[k, 2] = unit(k, up, 1).astype(BF16)
        firsts[k][2] = first_stage(k, 2, moved(dim, 1))
        s1[k, 3] = unit(k, down, 0).astype(BF16)
        firsts[k][3] = first_stage(k, 3, moved(dim, 3))
    for k in range(3):
        dim = orders[k][0]
        up, down = lax.rem(here[dim] + 1, 4), lax.rem(here[dim] + 3, 4)
        keep[k, 0] = unit(k, up, 0)
        keep[k, 1] = unit(k, down, 1)
    for k in range(3):
        for half in range(2):
            acc[k, half] = unit(k, here[orders[k][0]], half)
    for k in range(3):
        dim = orders[k][0]
        for half in range(2):
            firsts[k][half].wait_recv()
            s1[k, 4 + half] = (keep[k, half] + r1[k, half].astype(F32)).astype(BF16)
            firsts[k][4 + half] = first_stage(k, 4 + half, moved(dim, 1 if half == 0 else 3))
    for k in range(3):
        for message in (2, 3):
            firsts[k][message].wait_recv()
        acc[k, 0] = acc[k, 0] + r1[k, 3].astype(F32)
        acc[k, 1] = acc[k, 1] + r1[k, 2].astype(F32)

    seconds = [[None] * 3 for _ in range(3)]
    for k in range(3):
        dim = orders[k][1]
        for half in range(2):
            firsts[k][4 + half].wait_recv()
            acc[k, half] = acc[k, half] + r1[k, 4 + half].astype(F32)

    def stage_two(k, place):
        if k == 0:
            return acc[0, :, pl.ds(place * 2, 2)].reshape(4, PAD, 256)
        if k == 1:
            hi, lo = lax.div(place, 2), lax.rem(place, 2)
            return jnp.stack([acc[1, hi, 2 * cy + lo] for cy in range(4)])
        hi, lo = lax.div(place, 2), lax.rem(place, 2)
        return acc[2, hi, pl.ds(lo * 4, 4)]

    for k in range(3):
        dim = orders[k][1]
        for i, by in enumerate((2, 1, 3)):
            s2[k, i] = stage_two(k, lax.rem(here[dim] + by, 4)).astype(BF16)
            seconds[k][i] = send(s2.at[k, i], r2.at[k, i], S2 + 3 * k + i, moved(dim, by))
    for k in range(3):
        total = stage_two(k, here[orders[k][1]])
        for i in range(3):
            seconds[k][i].wait_recv()
            total = total + r2[k, i].astype(F32)
        keep[k, 0, 0:4] = total

    thirds = [[None] * 3 for _ in range(3)]
    for k in range(3):
        dim = orders[k][2]
        for i, by in enumerate((2, 1, 3)):
            s3[k, i] = keep[k, 0, lax.rem(here[dim] + by, 4)].astype(BF16)
            thirds[k][i] = send(s3.at[k, i], r3.at[k, i], S3 + 3 * k + i, moved(dim, by))
    for k in range(3):
        total = keep[k, 0, here[orders[k][2]]]
        for i in range(3):
            thirds[k][i].wait_recv()
            total = total + r3[k, i].astype(F32)
        out_ref[:, STARTS[k] : STARTS[k] + WIDTHS[k]] = (total * scaling)[:ROWS, : WIDTHS[k]]
    for copy in sent:
        copy.wait_send()


def solution(mesh):
    devices = mesh.shape["dp"] * mesh.shape["tensor"]

    def step(expert_act, grad_out, slot_token, slot_prob, live_count):
        slots, hidden = expert_act.shape
        tokens, features = grad_out.shape
        scaling = 1.0 / math.sqrt(slots * devices)
        blocks = (4, 4, 2, PAD)
        vmem = lambda *shape: pltpu.VMEM(shape, BF16)
        vmem32 = lambda *shape: pltpu.VMEM(shape, F32)
        return pl.pallas_call(
            functools.partial(kernel, scaling),
            out_shape=jax.ShapeDtypeStruct((ROWS, HALF), F32),
            in_specs=[
                pl.BlockSpec(memory_space=pltpu.VMEM),
                pl.BlockSpec(memory_space=pltpu.VMEM),
                pl.BlockSpec(memory_space=pltpu.SMEM),
                pl.BlockSpec(memory_space=pl.ANY),
                pl.BlockSpec(memory_space=pl.ANY),
            ],
            out_specs=pl.BlockSpec(memory_space=pltpu.VMEM),
            scratch_shapes=[
                vmem(hidden, slots), vmem(features, tokens), vmem(tokens, slots),
                vmem(2, *blocks, slots), vmem(*blocks, slots),
                vmem(3, 2, 256, slots), vmem(3, 2, 256, slots),
                vmem(3, 6, 8, PAD, 256), vmem(3, 6, 8, PAD, 256),
                vmem32(3, 2, 8, PAD, 256), vmem32(3, 2, 8, PAD, 256),
                vmem(3, 3, 4, PAD, 256), vmem(3, 3, 4, PAD, 256),
                vmem(3, 3, PAD, 256), vmem(3, 3, PAD, 256),
                pltpu.SemaphoreType.DMA((2,)),
                pltpu.SemaphoreType.DMA((N_MSG,)),
                pltpu.SemaphoreType.DMA((N_MSG,)),
            ],
            compiler_params=pltpu.CompilerParams(collective_id=0, has_side_effects=True),
        )(slot_token.reshape(1, slots), slot_prob.reshape(1, slots), live_count, expert_act.T, grad_out.T)

    both = ("dp", "tensor")
    return jax.shard_map(
        step,
        mesh=mesh,
        in_specs=(P(both, None), P(both, None), P(both), P(both), P(both)),
        out_specs=P("dp", "tensor"),
        check_vma=False,
    )
```

```python
import math

import jax
import jax.numpy as jnp
from jax import lax
from jax.experimental import pallas as pl
from jax.experimental.pallas import tpu as pltpu
from jax.sharding import PartitionSpec as P

MESH = pl.DeviceIdType.MESH
F32, BF16 = jnp.float32, jnp.bfloat16
ROWS, PAD = 45, 48
WIDTHS = (256, 256, 208)
STARTS = (0, 256, 512)
HALF = 720
VMEM_LIMIT = 55000000
LANES = 128
A_MSG, W_MSG, S1, S2, S3, N_MSG = 0, 4, 7, 43, 61, 79


def nt(left, right):
    return lax.dot_general(left, right, (((1,), (1,)), ((), ())), preferred_element_type=F32)


def kernel(
    live_ref, tok_hbm, prob_hbm, a_hbm, g_hbm, out_ref,
    tok_ref, prob_ref, a_v, g_v, hot, ap, ao, wp, wo, s1, r1, keep, acc, s2, r2, s3, r3,
    load_sem, send_sem, recv_sem,
):
    dp, x_hi = lax.axis_index("dp"), lax.axis_index("tensor")
    core = lax.rem(dp, 2)
    x_lo = lax.rem(lax.div(dp, 2), 2)
    z = lax.rem(lax.div(dp, 4), 4)
    y = lax.div(dp, 16)
    x = x_hi * 2 + x_lo

    def at(cx, cy, cz, cc):
        return (((cy * 4 + cz) * 2 + lax.rem(cx, 2)) * 2 + cc, lax.div(cx, 2))

    def moved(dim, by):
        place = {"x": x, "y": y, "z": z}
        place[dim] = lax.rem(place[dim] + by, 4)
        return at(place["x"], place["y"], place["z"], core)

    partner = at(x, y, z, 1 - core)
    here = {"x": x, "y": y, "z": z}
    orders = ("yzx", "zxy", "xyz")

    chunk = a_v.shape[0] // 4
    loads = [(a_hbm.at[pl.ds(i * chunk, chunk)], a_v.at[pl.ds(i * chunk, chunk)]) for i in range(4)]
    loads += [(tok_hbm, tok_ref), (prob_hbm, prob_ref)]
    loads += [(g_hbm.at[pl.ds(i * HALF, HALF)], g_v.at[pl.ds(i * HALF, HALF)]) for i in range(2)]
    loads = [pltpu.make_async_copy(src, dst, load_sem.at[i]) for i, (src, dst) in enumerate(loads)]
    for load in loads:
        load.start()

    barrier = pltpu.get_barrier_semaphore()
    peers = [partner] + [moved(d, by) for d in "xyz" for by in (1, 2, 3)]
    for peer in peers:
        pl.semaphore_signal(barrier, inc=1, device_id=peer, device_id_type=MESH)

    sent = []

    def send(src, dst, index, device):
        copy = pltpu.make_async_remote_copy(
            src_ref=src, dst_ref=dst, send_sem=send_sem.at[index], recv_sem=recv_sem.at[index],
            device_id=device, device_id_type=MESH,
        )
        copy.start()
        sent.append(copy)
        return copy

    tokens, slots = hot.shape
    zeros = jnp.zeros((PAD - ROWS, slots), F32)

    def padded(quarter):
        for parity in range(2):
            for q in range(8):
                first = ROWS * (16 * quarter + 2 * q + parity)
                base = first // 8 * 8
                stop = min(base + 56, (quarter + 1) * chunk)
                block = a_v[base:stop, :].astype(F32)[first - base : first - base + ROWS]
                block = jnp.concatenate([block, zeros], axis=0)
                ap[parity, quarter, q // 2, q % 2] = block.astype(BF16)

    a_copies = []
    for quarter in range(4):
        with jax.named_scope(f"pad{quarter}"):
            loads[quarter].wait()
            padded(quarter)
        if quarter == 0:
            with jax.named_scope("barrier"):
                pl.semaphore_wait(barrier, len(peers))
        a_copies.append(send(ap.at[1 - core, quarter], ao.at[quarter], A_MSG + quarter, partner))

    with jax.named_scope("hot"):
        loads[4].wait()
        loads[5].wait()
        for start in range(0, tokens, 256):
            rows = lax.broadcasted_iota(jnp.int32, (256, slots), 0) + start
            hot[start : start + 256, :] = (rows == tok_ref[...]).astype(F32).astype(BF16)
        position = lax.broadcasted_iota(jnp.int32, (1, slots), 1)
        weighting = jnp.where(position < live_ref[0], prob_ref[...], jnp.zeros((1, slots), F32))

    with jax.named_scope("weighted"):
        loads[6].wait()
        loads[7].wait()
        w_copies = []
        for k in range(3):
            width = WIDTHS[k]
            for half in range(2):
                first = half * HALF + STARTS[k]
                picked = jnp.dot(g_v[first : first + width, :], hot[...], preferred_element_type=F32)
                wp[k, half, :width, :] = (picked * weighting).astype(BF16)
                if width < 256:
                    wp[k, half, width:, :] = jnp.zeros((256 - width, slots), BF16)
            w_copies.append(send(wp.at[k], wo.at[k], W_MSG + k, partner))

    with jax.named_scope("swap_a"):
        for copy in a_copies:
            copy.wait_recv()

    def unit(k, place, half):
        if k == 0:
            own, other, right = ap[core, place], ao[place], (k, half)
        elif k == 1:
            own, other, right = ap[core, :, place], ao[:, place], (k, half)
        else:
            low = lax.rem(place, 2)
            own = ap[core, 2 * half : 2 * half + 2, :, low]
            other = ao[2 * half : 2 * half + 2, :, low]
            right = (k, lax.div(place, 2))
        own, other = own.reshape(8 * PAD, slots), other.reshape(8 * PAD, slots)
        return (nt(own, wp[right]) + nt(other, wo[right])).reshape(8, PAD, 256)

    def first_stage(k, part, message, device):
        index = S1 + (k * 2 + part) * 6 + message
        return send(s1.at[k, part, message], r1.at[k, part, message], index, device)

    def both_parts(k, message, value):
        for part in range(2):
            s1[k, part, message] = value[:, :, lanes(part)].astype(BF16)

    def lanes(part):
        return slice(part * LANES, part * LANES + LANES)

    firsts = [[[None] * 6 for _ in range(2)] for _ in range(3)]
    ends = []
    for k in range(3):
        dim = orders[k][0]
        far, up, down = [lax.rem(here[dim] + by, 4) for by in (2, 1, 3)]
        ends.append((dim, far, up, down))
    for k, (dim, far, _, _) in enumerate(ends):
        with jax.named_scope(f"swap_w{k}"):
            w_copies[k].wait_recv()
        with jax.named_scope(f"m1_{k}"):
            for half in range(2):
                both_parts(k, half, unit(k, far, half))
            for part in range(2):
                for half in range(2):
                    firsts[k][part][half] = first_stage(k, part, half, moved(dim, 1 + 2 * half))
    with jax.named_scope("m2"):
        for k, (dim, _, up, down) in enumerate(ends):
            both_parts(k, 2, unit(k, up, 1))
            both_parts(k, 3, unit(k, down, 0))
        for part in range(2):
            for k, (dim, _, up, down) in enumerate(ends):
                firsts[k][part][2] = first_stage(k, part, 2, moved(dim, 1))
                firsts[k][part][3] = first_stage(k, part, 3, moved(dim, 3))
    with jax.named_scope("keep"):
        for k, (dim, _, up, down) in enumerate(ends):
            keep[k, 0] = unit(k, up, 0)
            keep[k, 1] = unit(k, down, 1)
    with jax.named_scope("own"):
        for k, (dim, _, _, _) in enumerate(ends):
            for half in range(2):
                acc[k, half] = unit(k, here[dim], half)
    for part in range(2):
        cols = lanes(part)
        for k, (dim, _, _, _) in enumerate(ends):
            with jax.named_scope(f"m3_{part}{k}"):
                for half in range(2):
                    firsts[k][part][half].wait_recv()
                    s1[k, part, 4 + half] = (keep[k, half, :, :, cols] + r1[k, part, half].astype(F32)).astype(BF16)
                for half in range(2):
                    firsts[k][part][4 + half] = first_stage(k, part, 4 + half, moved(dim, 1 + 2 * half))

    def stage_two(k, place, cols):
        if k == 0:
            return acc[0, :, pl.ds(place * 2, 2), :, cols].reshape(4, PAD, LANES)
        hi, lo = lax.div(place, 2), lax.rem(place, 2)
        if k == 1:
            return jnp.stack([acc[1, hi, 2 * cy + lo, :, cols] for cy in range(4)])
        return acc[2, hi, pl.ds(lo * 4, 4), :, cols]

    seconds, thirds = {}, {}
    for part in range(2):
        cols = lanes(part)
        for k in range(3):
            dim = orders[k][1]
            with jax.named_scope(f"m2_wait_{part}{k}"):
                for message in (2, 3):
                    firsts[k][part][message].wait_recv()
                acc[k, 0, :, :, cols] = acc[k, 0, :, :, cols] + r1[k, part, 3].astype(F32)
                acc[k, 1, :, :, cols] = acc[k, 1, :, :, cols] + r1[k, part, 2].astype(F32)
        for k in range(3):
            dim = orders[k][1]
            with jax.named_scope(f"m3_wait_{part}{k}"):
                for half in range(2):
                    firsts[k][part][4 + half].wait_recv()
                    acc[k, half, :, :, cols] = acc[k, half, :, :, cols] + r1[k, part, 4 + half].astype(F32)
            with jax.named_scope(f"s2_send_{part}{k}"):
                for i, by in enumerate((2, 1, 3)):
                    s2[k, part, i] = stage_two(k, lax.rem(here[dim] + by, 4), cols).astype(BF16)
                for i, by in enumerate((2, 1, 3)):
                    seconds[k, part, i] = send(
                        s2.at[k, part, i], r2.at[k, part, i], S2 + 6 * k + 3 * part + i, moved(dim, by)
                    )
    for part in range(2):
        cols = lanes(part)
        for k in range(3):
            dim = orders[k][2]
            with jax.named_scope(f"s2_wait_{part}{k}"):
                total = stage_two(k, here[orders[k][1]], cols)
                for i in range(3):
                    seconds[k, part, i].wait_recv()
                    total = total + r2[k, part, i].astype(F32)
                keep[k, part, 0:4, :, :LANES] = total
            with jax.named_scope(f"s3_send_{part}{k}"):
                for i, by in enumerate((2, 1, 3)):
                    s3[k, part, i] = keep[k, part, lax.rem(here[dim] + by, 4), :, :LANES].astype(BF16)
                for i, by in enumerate((2, 1, 3)):
                    thirds[k, part, i] = send(
                        s3.at[k, part, i], r3.at[k, part, i], S3 + 6 * k + 3 * part + i, moved(dim, by)
                    )
    for part in range(2):
        for k in range(3):
            with jax.named_scope(f"s3_wait_{part}{k}"):
                total = keep[k, part, here[orders[k][2]], :, :LANES]
                for i in range(3):
                    thirds[k, part, i].wait_recv()
                    total = total + r3[k, part, i].astype(F32)
                first = STARTS[k] + part * LANES
                last = min(first + LANES, STARTS[k] + WIDTHS[k])
                out_ref[:, first:last] = total[:ROWS, : last - first]
    with jax.named_scope('drain'):
        for copy in sent:
            copy.wait_send()


def solution(mesh):
    devices = mesh.shape["dp"] * mesh.shape["tensor"]

    def step(expert_act, grad_out, slot_token, slot_prob, live_count):
        slots, hidden = expert_act.shape
        tokens, features = grad_out.shape
        scaling = 1.0 / math.sqrt(slots * devices)
        blocks = (4, 4, 2, PAD)
        vmem = lambda *shape: pltpu.VMEM(shape, BF16)
        vmem32 = lambda *shape: pltpu.VMEM(shape, F32)
        gradient = pl.pallas_call(
            kernel,
            out_shape=jax.ShapeDtypeStruct((ROWS, HALF), F32),
            in_specs=[
                pl.BlockSpec(memory_space=pltpu.SMEM),
                *[pl.BlockSpec(memory_space=pltpu.HBM)] * 4,
            ],
            out_specs=pl.BlockSpec(memory_space=pltpu.VMEM),
            scratch_shapes=[
                pltpu.VMEM((1, slots), jnp.int32), vmem32(1, slots),
                vmem(hidden, slots), vmem(features, tokens), vmem(tokens, slots),
                vmem(2, *blocks, slots), vmem(*blocks, slots),
                vmem(3, 2, 256, slots), vmem(3, 2, 256, slots),
                vmem(3, 2, 6, 8, PAD, LANES), vmem(3, 2, 6, 8, PAD, LANES),
                vmem32(3, 2, 8, PAD, 256), vmem32(3, 2, 8, PAD, 256),
                vmem(3, 2, 3, 4, PAD, LANES), vmem(3, 2, 3, 4, PAD, LANES),
                vmem(3, 2, 3, PAD, LANES), vmem(3, 2, 3, PAD, LANES),
                pltpu.SemaphoreType.DMA((8,)),
                pltpu.SemaphoreType.DMA((N_MSG,)),
                pltpu.SemaphoreType.DMA((N_MSG,)),
            ],
            compiler_params=pltpu.CompilerParams(collective_id=0, has_side_effects=True, vmem_limit_bytes=VMEM_LIMIT),
        )(live_count, slot_token.reshape(1, slots), slot_prob.reshape(1, slots), expert_act.T, grad_out.T)
        return gradient * scaling

    both = ("dp", "tensor")
    return jax.shard_map(
        step,
        mesh=mesh,
        in_specs=(P(both, None), P(both, None), P(both), P(both), P(both)),
        out_specs=P("dp", "tensor"),
        check_vma=False,
    )
```

```python
import math

import jax
import jax.numpy as jnp
from jax import lax
from jax.experimental import pallas as pl
from jax.experimental.pallas import tpu as pltpu
from jax.sharding import PartitionSpec as P

MESH = pl.DeviceIdType.MESH
F32, BF16 = jnp.float32, jnp.bfloat16
ROWS, PAD = 45, 48
WIDTHS = (256, 256, 208)
STARTS = (0, 256, 512)
HALF = 720
VMEM_LIMIT = 60 * 1024 * 1024
LANES = 128
A_IN, W_IN, FAR, NEAR, RELAY, SECOND, THIRD, N_IN = 0, 1, 4, 7, 10, 16, 22, 28
A_OUT, W_OUT, FAR_OUT, NEAR_OUT, RELAY_OUT, SECOND_OUT, THIRD_OUT, N_OUT = 0, 1, 2, 3, 4, 5, 6, 7


def nt(left, right):
    return lax.dot_general(left, right, (((1,), (1,)), ((), ())), preferred_element_type=F32)


def kernel(
    live_ref, tok_hbm, prob_hbm, a_hbm, g_hbm, out_ref,
    tok_ref, prob_ref, a_v, g_v, hot, ap, ao, wp, wo, sf, rf, sn, rn, sr, rr, keep, acc, s2, r2, s3, r3,
    load_sem, send_sem, recv_sem,
):
    dp, x_hi = lax.axis_index("dp"), lax.axis_index("tensor")
    core = lax.rem(dp, 2)
    x_lo = lax.rem(lax.div(dp, 2), 2)
    z = lax.rem(lax.div(dp, 4), 4)
    y = lax.div(dp, 16)
    x = x_hi * 2 + x_lo

    def at(cx, cy, cz, cc):
        return (((cy * 4 + cz) * 2 + lax.rem(cx, 2)) * 2 + cc, lax.div(cx, 2))

    def moved(dim, by):
        place = {"x": x, "y": y, "z": z}
        place[dim] = lax.rem(place[dim] + by, 4)
        return at(place["x"], place["y"], place["z"], core)

    partner = at(x, y, z, 1 - core)
    here = {"x": x, "y": y, "z": z}
    orders = ("yzx", "zxy", "xyz")

    chunk = a_v.shape[0] // 4
    loads = [(a_hbm.at[pl.ds(i * chunk, chunk)], a_v.at[pl.ds(i * chunk, chunk)]) for i in range(4)]
    loads += [(tok_hbm, tok_ref), (prob_hbm, prob_ref)]
    loads += [(g_hbm.at[pl.ds(i * HALF, HALF)], g_v.at[pl.ds(i * HALF, HALF)]) for i in range(2)]
    loads = [pltpu.make_async_copy(src, dst, load_sem.at[i]) for i, (src, dst) in enumerate(loads)]
    for load in loads:
        load.start()

    barrier = pltpu.get_barrier_semaphore()
    peers = [partner] + [moved(d, by) for d in "xyz" for by in (1, 2, 3)]
    for peer in peers:
        pl.semaphore_signal(barrier, inc=1, device_id=peer, device_id_type=MESH)

    def copy(src, dst, out, into, device):
        return pltpu.make_async_remote_copy(
            src_ref=src, dst_ref=dst, send_sem=send_sem.at[out], recv_sem=recv_sem.at[into],
            device_id=device, device_id_type=MESH,
        )

    def send(src, dst, out, into, device):
        copy(src, dst, out, into, device).start()

    def arrived(src, dst, out, into):
        copy(src, dst, out, into, partner).wait_recv()

    tokens, slots = hot.shape
    zeros = jnp.zeros((PAD - ROWS, slots), F32)

    def padded(quarter):
        for parity in range(2):
            for q in range(8):
                first = ROWS * (16 * quarter + 2 * q + parity)
                base = first // 8 * 8
                stop = min(base + 56, (quarter + 1) * chunk)
                block = a_v[base:stop, :].astype(F32)[first - base : first - base + ROWS]
                block = jnp.concatenate([block, zeros], axis=0)
                ap[parity, quarter, q // 2, q % 2] = block.astype(BF16)

    for quarter in range(4):
        with jax.named_scope(f"pad{quarter}"):
            loads[quarter].wait()
            padded(quarter)
        if quarter == 0:
            with jax.named_scope("barrier"):
                pl.semaphore_wait(barrier, len(peers))
        send(ap.at[1 - core, quarter], ao.at[quarter], A_OUT, A_IN, partner)

    with jax.named_scope("hot"):
        loads[4].wait()
        loads[5].wait()
        for start in range(0, tokens, 256):
            rows = lax.broadcasted_iota(jnp.int32, (256, slots), 0) + start
            hot[start : start + 256, :] = (rows == tok_ref[...]).astype(F32).astype(BF16)
        position = lax.broadcasted_iota(jnp.int32, (1, slots), 1)
        weighting = jnp.where(position < live_ref[0], prob_ref[...], jnp.zeros((1, slots), F32))

    with jax.named_scope("weighted"):
        loads[6].wait()
        loads[7].wait()
        for k in range(3):
            width = WIDTHS[k]
            for half in range(2):
                first = half * HALF + STARTS[k]
                picked = jnp.dot(g_v[first : first + width, :], hot[...], preferred_element_type=F32)
                wp[k, half, :width, :] = (picked * weighting).astype(BF16)
                if width < 256:
                    wp[k, half, width:, :] = jnp.zeros((256 - width, slots), BF16)
            send(wp.at[k], wo.at[k], W_OUT, W_IN + k, partner)

    with jax.named_scope("swap_a"):
        arrived(ap.at[0], ao, A_OUT, A_IN)

    def unit(k, place, half):
        if k == 0:
            own, other, right = ap[core, place], ao[place], (k, half)
        elif k == 1:
            own, other, right = ap[core, :, place], ao[:, place], (k, half)
        else:
            low = lax.rem(place, 2)
            own = ap[core, 2 * half : 2 * half + 2, :, low]
            other = ao[2 * half : 2 * half + 2, :, low]
            right = (k, lax.div(place, 2))
        own, other = own.reshape(8 * PAD, slots), other.reshape(8 * PAD, slots)
        return (nt(own, wp[right]) + nt(other, wo[right])).reshape(8, PAD, 256)

    def lanes(part):
        return slice(part * LANES, part * LANES + LANES)

    ends = []
    for k in range(3):
        dim = orders[k][0]
        far, up, down = [lax.rem(here[dim] + by, 4) for by in (2, 1, 3)]
        ends.append((far, up, down, (moved(dim, 1), moved(dim, 3))))
    for k, (far, _, _, sides) in enumerate(ends):
        with jax.named_scope(f"swap_w{k}"):
            arrived(wp.at[k], wo.at[k], W_OUT, W_IN + k)
        with jax.named_scope(f"m1_{k}"):
            for half in range(2):
                sf[k, half] = unit(k, far, half).astype(BF16)
            for half in range(2):
                send(sf.at[k, half], rf.at[k, half], FAR_OUT, FAR + k, sides[half])
    with jax.named_scope("m2"):
        for k, (_, up, down, sides) in enumerate(ends):
            sn[k, 0] = unit(k, up, 1).astype(BF16)
            sn[k, 1] = unit(k, down, 0).astype(BF16)
        for k, (_, _, _, sides) in enumerate(ends):
            for side in range(2):
                send(sn.at[k, side], rn.at[k, side], NEAR_OUT, NEAR + k, sides[side])
    with jax.named_scope("keep"):
        for k, (_, up, down, _) in enumerate(ends):
            keep[k, 0] = unit(k, up, 0)
            keep[k, 1] = unit(k, down, 1)
    with jax.named_scope("own"):
        for k in range(3):
            for half in range(2):
                acc[k, half] = unit(k, here[orders[k][0]], half)
    for part in range(2):
        cols = lanes(part)
        for k, (_, _, _, sides) in enumerate(ends):
            with jax.named_scope(f"m3_{part}{k}"):
                if part == 0:
                    arrived(sf.at[k], rf.at[k], FAR_OUT, FAR + k)
                for half in range(2):
                    sr[k, part, half] = (keep[k, half, :, :, cols] + rf[k, half, :, :, cols].astype(F32)).astype(BF16)
                for half in range(2):
                    send(sr.at[k, part, half], rr.at[k, part, half], RELAY_OUT, RELAY + 2 * k + part, sides[half])

    def stage_two(k, place, cols):
        if k == 0:
            return acc[0, :, pl.ds(place * 2, 2), :, cols].reshape(4, PAD, LANES)
        hi, lo = lax.div(place, 2), lax.rem(place, 2)
        if k == 1:
            return jnp.stack([acc[1, hi, 2 * cy + lo, :, cols] for cy in range(4)])
        return acc[2, hi, pl.ds(lo * 4, 4), :, cols]

    for k in range(3):
        with jax.named_scope(f"m2_wait_{k}"):
            arrived(sn.at[k], rn.at[k], NEAR_OUT, NEAR + k)
            for half in range(2):
                acc[k, half] = acc[k, half] + rn[k, 1 - half].astype(F32)
    for part in range(2):
        cols = lanes(part)
        for k in range(3):
            dim = orders[k][1]
            with jax.named_scope(f"m3_wait_{part}{k}"):
                arrived(sr.at[k, part], rr.at[k, part], RELAY_OUT, RELAY + 2 * k + part)
                for half in range(2):
                    acc[k, half, :, :, cols] = acc[k, half, :, :, cols] + rr[k, part, half].astype(F32)
            with jax.named_scope(f"s2_send_{part}{k}"):
                for i, by in enumerate((2, 1, 3)):
                    s2[k, part, i] = stage_two(k, lax.rem(here[dim] + by, 4), cols).astype(BF16)
                for i, by in enumerate((2, 1, 3)):
                    send(s2.at[k, part, i], r2.at[k, part, i], SECOND_OUT, SECOND + 2 * k + part, moved(dim, by))
    for part in range(2):
        cols = lanes(part)
        for k in range(3):
            dim = orders[k][2]
            with jax.named_scope(f"s2_wait_{part}{k}"):
                total = stage_two(k, here[orders[k][1]], cols)
                arrived(s2.at[k, part], r2.at[k, part], SECOND_OUT, SECOND + 2 * k + part)
                for i in range(3):
                    total = total + r2[k, part, i].astype(F32)
                keep[k, part, 0:4, :, :LANES] = total
            with jax.named_scope(f"s3_send_{part}{k}"):
                for i, by in enumerate((2, 1, 3)):
                    s3[k, part, i] = keep[k, part, lax.rem(here[dim] + by, 4), :, :LANES].astype(BF16)
                for i, by in enumerate((2, 1, 3)):
                    send(s3.at[k, part, i], r3.at[k, part, i], THIRD_OUT, THIRD + 2 * k + part, moved(dim, by))
    for part in range(2):
        for k in range(3):
            with jax.named_scope(f"s3_wait_{part}{k}"):
                total = keep[k, part, here[orders[k][2]], :, :LANES]
                arrived(s3.at[k, part], r3.at[k, part], THIRD_OUT, THIRD + 2 * k + part)
                for i in range(3):
                    total = total + r3[k, part, i].astype(F32)
                first = STARTS[k] + part * LANES
                last = min(first + LANES, STARTS[k] + WIDTHS[k])
                out_ref[:, first:last] = total[:ROWS, : last - first]
    with jax.named_scope("drain"):
        leaving = ((ap.at[0], ao), (wp, wo), (sf, rf), (sn, rn), (sr, rr), (s2, r2), (s3, r3))
        for out, (src, dst) in enumerate(leaving):
            copy(src, dst, out, 0, partner).wait_send()


def solution(mesh):
    devices = mesh.shape["dp"] * mesh.shape["tensor"]

    def step(expert_act, grad_out, slot_token, slot_prob, live_count):
        slots, hidden = expert_act.shape
        tokens, features = grad_out.shape
        scaling = 1.0 / math.sqrt(slots * devices)
        blocks = (4, 4, 2, PAD)
        vmem = lambda *shape: pltpu.VMEM(shape, BF16)
        vmem32 = lambda *shape: pltpu.VMEM(shape, F32)
        gradient = pl.pallas_call(
            kernel,
            out_shape=pltpu.VMEM((ROWS, HALF), F32),
            in_specs=[
                pl.BlockSpec(memory_space=pltpu.SMEM),
                *[pl.BlockSpec(memory_space=pltpu.HBM)] * 4,
            ],
            out_specs=pl.BlockSpec(memory_space=pltpu.VMEM),
            scratch_shapes=[
                pltpu.VMEM((1, slots), jnp.int32), vmem32(1, slots),
                vmem(hidden, slots), vmem(features, tokens), vmem(tokens, slots),
                vmem(2, *blocks, slots), vmem(*blocks, slots),
                vmem(3, 2, 256, slots), vmem(3, 2, 256, slots),
                vmem(3, 2, 8, PAD, 256), vmem(3, 2, 8, PAD, 256),
                vmem(3, 2, 8, PAD, 256), vmem(3, 2, 8, PAD, 256),
                vmem(3, 2, 2, 8, PAD, LANES), vmem(3, 2, 2, 8, PAD, LANES),
                vmem32(3, 2, 8, PAD, 256), vmem32(3, 2, 8, PAD, 256),
                vmem(3, 2, 3, 4, PAD, LANES), vmem(3, 2, 3, 4, PAD, LANES),
                vmem(3, 2, 3, PAD, LANES), vmem(3, 2, 3, PAD, LANES),
                pltpu.SemaphoreType.DMA((8,)),
                pltpu.SemaphoreType.DMA((N_OUT,)),
                pltpu.SemaphoreType.DMA((N_IN,)),
            ],
            compiler_params=pltpu.CompilerParams(collective_id=0, has_side_effects=True, vmem_limit_bytes=VMEM_LIMIT),
        )(live_count, slot_token.reshape(1, slots), slot_prob.reshape(1, slots), expert_act.T, grad_out.T)
        return gradient * scaling

    both = ("dp", "tensor")
    return jax.shard_map(
        step,
        mesh=mesh,
        in_specs=(P(both, None), P(both, None), P(both), P(both), P(both)),
        out_specs=P("dp", "tensor"),
        check_vma=False,
    )
```
